32 devices in a mesh: blk: 8 (over z, y), rep: 4 (over x, core).
Axes of the slice: x: 2, y: 2, z: 4, core: 2. Of those that a mesh axis runs over, the one named last changes fastest.
Arguments:
- tokens: bfloat16 [4096, 8192], P(('blk', 'rep')), may hold values from -6 to 6
- gate_weight: bfloat16 [8, 8192], P('blk'), may hold values from -0.0625 to 0.0625
- up_weight: bfloat16 [8, 8192], P('blk'), may hold values from -0.0625 to 0.0625
- down_weight: bfloat16 [8, 8192], P('blk'), may hold values from -2 to 2
Outputs:
- grad_gate: float32 [8, 8192], P('blk')
- grad_up: float32 [8, 8192], P('blk')
- grad_down: float32 [8, 8192], P('blk')
The draws below stay inside these ranges and needn't reach their ends.
All inputs are finite; a program needn't handle non-finite values.
Results may differ from the reference program's by a relative error of at most 0.0027.
Values may be sent and summed in bfloat16 or wider, within the bound.
A program may use at most 64 MiB of HBM per device.

```python
import math
import jax
import jax.numpy as jnp
from jax import lax

D = 8192
HIDW = 8
TOKENS = 4096


def steps_of(stream_key, dims, shards, low, largest):
    loudness, own = 1.0, jax.random.fold_in(stream_key, 6)
    for axis_at, parts in shards:
        heights = jnp.exp(jax.random.uniform(jax.random.fold_in(own, axis_at), (parts,), jnp.float32, low / len(shards), largest / len(shards)))
        loudness = loudness * jnp.repeat(heights, dims[axis_at] // parts).reshape([-1 if axis == axis_at else 1 for axis in range(len(dims))])
    return loudness


def gaussian(stream_key, shape, scale, most, shards=(), held_as=jnp.bfloat16):
    drawn = scale * jax.random.normal(stream_key, shape, jnp.float32)
    if shards:
        drawn = drawn * steps_of(stream_key, shape, shards, -0.22, 0.18)
    return jnp.clip(drawn, -most, most).astype(held_as)


def setup_inputs(seed: int = 0) -> dict:
    arg_keys = jax.random.split(jax.random.key(seed), 5)
    tokens = gaussian(arg_keys[0], (TOKENS, D), 1.0, 6.0, ((0, 32),))
    gate_weight = gaussian(arg_keys[1], (HIDW, D), D ** -0.5, 0.0625, ((0, 8),))
    up_weight = gaussian(arg_keys[2], (HIDW, D), D ** -0.5, 0.0625, ((0, 8),))
    down_weight = gaussian(arg_keys[3], (HIDW, D), HIDW ** -0.5, 2.0, ((0, 8),))
    return {"tokens": tokens, "gate_weight": gate_weight, "up_weight": up_weight, "down_weight": down_weight}


def reference(tokens, gate_weight, up_weight, down_weight):
    loss_scale = float(TOKENS) ** -0.5
    block_rows = math.gcd(TOKENS, 2048)
    blocked = tokens.reshape(TOKENS // block_rows, block_rows, D)

    def accumulate(totals, rows):
        gate_pre = jnp.dot(rows, gate_weight.T, preferred_element_type=jnp.float32)
        up_pre = jnp.dot(rows, up_weight.T, preferred_element_type=jnp.float32)
        sigmoid_gate = jax.nn.sigmoid(gate_pre)
        active = gate_pre * sigmoid_gate
        hidden = (active * up_pre).astype(jnp.bfloat16)
        layer_out = jnp.dot(hidden, down_weight, preferred_element_type=jnp.float32)
        cotangent = (layer_out * loss_scale).astype(jnp.bfloat16)
        hidden_grad = jnp.dot(cotangent, down_weight.T, preferred_element_type=jnp.float32)
        gate_grad = (hidden_grad * up_pre * (sigmoid_gate * (1.0 + gate_pre * (1.0 - sigmoid_gate)))).astype(jnp.bfloat16)
        up_grad = (hidden_grad * active).astype(jnp.bfloat16)
        new_gate = totals[0] + jnp.dot(gate_grad.T, rows, preferred_element_type=jnp.float32)
        new_up = totals[1] + jnp.dot(up_grad.T, rows, preferred_element_type=jnp.float32)
        new_down = totals[2] + jnp.dot(hidden.T, cotangent, preferred_element_type=jnp.float32)
        return (new_gate, new_up, new_down), None

    zeros = jnp.zeros((HIDW, D), jnp.float32)
    totals, unused = lax.scan(accumulate, (zeros, zeros, zeros), blocked)
    return (totals[0], totals[1], totals[2])
```

```python
import functools
import math

import jax
import jax.numpy as jnp
from jax import lax
from jax.experimental import pallas as pl
from jax.experimental.pallas import tpu as pltpu
from jax.sharding import PartitionSpec as P

F32, BF16 = jnp.float32, jnp.bfloat16
NT = (((1,), (1,)), ((), ()))
EXACT = lax.Precision.HIGHEST


def each(count, body):
    if count <= 32:
        for i in range(count):
            body(i)
    else:
        lax.fori_loop(0, count, lambda i, c: (body(i), c)[1], 0)


def kernel(
    B, R, PX, loss_scale,
    tok_hbm, gate_ref, up_ref, down_ref,
    out_gate, out_up, out_down,
    tok, rows_in, down_in, w_all, wd_all, gram, pair, partner_in, part, mine, send, recv, share,
    tok_sem, w_send, w_recv, d_send, d_recv, g_send, g_recv, p_send, p_recv, r_send, r_recv, o_send, o_recv,
):
    T, F = tok.shape
    XN = R // 2
    HW = F // 2
    PW = HW // PX
    me_b, me_r = lax.axis_index("blk"), lax.axis_index("rep")
    core, xi = lax.rem(me_r, 2), lax.div(me_r, 2)
    everyone = PX == XN

    def if_owner(body):
        if everyone:
            body()
        else:
            pl.when(xi < PX)(body)

    def remote(src, dst, ss, rs, b, r):
        return pltpu.make_async_remote_copy(
            src_ref=src, dst_ref=dst, send_sem=ss, recv_sem=rs,
            device_id={"blk": b, "rep": r}, device_id_type=pl.DeviceIdType.MESH,
        )

    load = pltpu.make_async_copy(tok_hbm, tok, tok_sem)
    load.start()

    barrier = pltpu.get_barrier_semaphore()

    def greet(b, r):
        pl.semaphore_signal(
            barrier, inc=1, device_id={"blk": b, "rep": r}, device_id_type=pl.DeviceIdType.MESH
        )

    def same_core(i):
        k = i + 1
        return lax.rem(me_b + k // XN, B), 2 * lax.rem(xi + k % XN, XN) + core

    each(B * XN - 1, lambda i: greet(*same_core(i)))
    each(XN, lambda i: greet(me_b, 2 * i + 1 - core))
    pl.semaphore_wait(barrier, B * XN - 1 + XN)

    my_col = pl.multiple_of(core * HW + lax.rem(xi, PX) * PW, 128)

    def d_copy(i):
        b = lax.rem(me_b + i + 1, B)
        return remote(
            down_ref.at[:, pl.ds(my_col, PW)], down_in.at[me_b], d_send.at[b], d_recv.at[me_b], b, me_r
        )

    def w_copy(which, ref, i):
        b = lax.rem(me_b + i + 1, B)
        return remote(ref, rows_in.at[which, me_b], w_send.at[which, b], w_recv.at[which, me_b], b, me_r)

    each(B - 1, lambda i: d_copy(i).start())
    each(B - 1, lambda i: (w_copy(0, gate_ref, i).start(), w_copy(1, up_ref, i).start()))

    down_in[me_b] = down_ref[:, pl.ds(my_col, PW)]
    rows_in[0, me_b] = gate_ref[...]
    rows_in[1, me_b] = up_ref[...]

    def d_arrived(i):
        b = lax.rem(me_b + i + 1, B)
        remote(down_in.at[b], down_in.at[b], d_send.at[b], d_recv.at[b], b, me_r).wait_recv()

    each(B - 1, d_arrived)
    for b in range(B):
        wd_all[b : b + 1, :] = down_in[b].astype(F32)

    def g_copy(i):
        r = lax.rem(me_r + i + 1, R)
        return remote(gram.at[me_r], gram.at[me_r], g_send.at[r], g_recv.at[me_r], me_b, r)

    def make_gram():
        wd = wd_all[...].astype(BF16)
        gram[me_r, :, :] = jnp.zeros(gram.shape[1:], F32)
        gram[me_r, :, 0:B] = lax.dot_general(wd, wd, NT, preferred_element_type=F32)
        each(R - 1, lambda i: g_copy(i).start())

    if_owner(make_gram)

    def w_arrived(i):
        b = lax.rem(me_b + i + 1, B)
        for which in range(2):
            slot = rows_in.at[which, b]
            remote(slot, slot, w_send.at[which, b], w_recv.at[which, b], b, me_r).wait_recv()

    each(B - 1, w_arrived)
    for which in range(2):
        for b in range(B):
            w_all[which * B + b : which * B + b + 1, :] = rows_in[which, b].astype(F32)

    load.wait()
    pre = lax.dot_general(w_all[...].astype(BF16), tok[...], NT, preferred_element_type=F32)
    gate_pre, up_pre = pre[:B], pre[B:]
    s = jax.nn.sigmoid(gate_pre)
    active = gate_pre * s
    hidden = (active * up_pre).astype(BF16)

    def g_arrived(i):
        r = lax.rem(me_r + i + 1, R)

        def wait():
            remote(gram.at[r], gram.at[r], g_send.at[r], g_recv.at[r], me_b, r).wait_recv()

        if everyone:
            wait()
        else:
            pl.when(r < 2 * PX)(wait)

    each(R - 1, g_arrived)
    gd = gram[0]
    for r in range(1, 2 * PX):
        gd = gd + gram[r]
    hidden_grad = loss_scale * jnp.dot(
        gd[:, :B], hidden.astype(F32), precision=EXACT, preferred_element_type=F32
    )
    pair[pl.ds(0, B, stride=2), :] = hidden_grad * up_pre * (s * (1.0 + gate_pre * (1.0 - s)))
    pair[pl.ds(1, B, stride=2), :] = hidden_grad * active
    lhs = pair[...].astype(BF16)

    chunk = math.gcd(512, PW)

    def half(which, ref):
        for c in range(0, HW, chunk):
            col = pl.multiple_of(which * HW + c, 128)
            ref[:, c : c + chunk] = jnp.dot(lhs, tok[:, pl.ds(col, chunk)], preferred_element_type=F32)

    half(1 - core, part)
    part[:, HW:] = jnp.zeros((2 * B, 128), F32)
    part[0:B, HW : HW + B] = lax.dot_general(hidden, hidden, NT, preferred_element_type=F32)
    partner = remote(part, partner_in, p_send, p_recv, me_b, 2 * xi + 1 - core)
    partner.start()
    half(core, mine)
    partner.wait_recv()

    ghat = part[0:B, HW:] + partner_in[0:B, HW:]
    ghi = ghat.astype(BF16).astype(F32)
    glo = ghat - ghi
    for b in range(B):
        gpair = jnp.concatenate([ghi[b : b + 1], glo[b : b + 1]], axis=0).astype(BF16)
        for q in range(PX):
            cols = slice(q * PW, (q + 1) * PW)
            term = mine[2 * b : 2 * b + 2, cols] + partner_in[2 * b : 2 * b + 2, cols]
            send[b, q, :, 0:PW] = term.astype(BF16)
            send[b, q, :, PW:] = gpair

    def r_copy(i):
        b, r = same_core(i)
        q = lax.div(r, 2)
        at = me_b * XN + xi
        qq = q if everyone else lax.rem(q, PX)
        return q, remote(send.at[b, qq], recv.at[at], r_send.at[b * XN + q], r_recv.at[at], b, r)

    def for_r(act):
        def body(i):
            q, copy = r_copy(i)
            if everyone:
                act(copy)
            else:
                pl.when(q < PX)(lambda: act(copy))

        each(B * XN - 1, body)

    for_r(lambda copy: copy.start())

    def o_copy(i):
        r = lax.rem(me_r + i + 1, R)
        return remote(share.at[me_r], share.at[me_r], o_send.at[r], o_recv.at[me_r], me_b, r)

    def r_arrived(i):
        b, r = same_core(i)
        at = b * XN + lax.div(r, 2)
        remote(recv.at[at], recv.at[at], r_send.at[at], r_recv.at[at], b, r).wait_recv()

    def finish():
        recv[me_b * XN + xi] = send[me_b, xi if everyone else lax.rem(xi, PX)]
        each(B * XN - 1, r_arrived)
        n = B * XN
        if n <= 32:
            total = recv[0].astype(F32)
            for i in range(1, n):
                total = total + recv[i].astype(F32)
        else:
            total = lax.fori_loop(
                1, n, lambda i, c: c + recv[i].astype(F32), recv[0].astype(F32)
            )
        share[me_r, 0:2, :] = total[:, 0:PW]
        grow = total[0:1, PW:] + total[1:2, PW:]
        eye = lax.broadcasted_iota(jnp.int32, (B, 128), 0) == lax.broadcasted_iota(jnp.int32, (B, 128), 1)
        gcol = jnp.sum(jnp.where(eye, jnp.broadcast_to(grow, (B, 128)), 0.0), axis=1, keepdims=True)
        share[me_r, 2:3, :] = loss_scale * jnp.sum(gcol * wd_all[...], axis=0, keepdims=True)
        each(R - 1, lambda i: o_copy(i).start())

    if_owner(finish)

    def o_arrived(i):
        r = lax.rem(me_r + i + 1, R)

        def wait():
            remote(share.at[r], share.at[r], o_send.at[r], o_recv.at[r], me_b, r).wait_recv()

        if everyone:
            wait()
        else:
            pl.when(r < 2 * PX)(wait)

    each(R - 1, o_arrived)
    for r in range(2 * PX):
        col = (r % 2) * HW + (r // 2) * PW
        out_gate[:, col : col + PW] = share[r, 0:1, :]
        out_up[:, col : col + PW] = share[r, 1:2, :]
        out_down[:, col : col + PW] = share[r, 2:3, :]

    each(B - 1, lambda i: d_copy(i).wait_send())
    each(B - 1, lambda i: (w_copy(0, gate_ref, i).wait_send(), w_copy(1, up_ref, i).wait_send()))
    if_owner(lambda: each(R - 1, lambda i: g_copy(i).wait_send()))
    partner.wait_send()
    for_r(lambda copy: copy.wait_send())
    if_owner(lambda: each(R - 1, lambda i: o_copy(i).wait_send()))


def solution(mesh):
    B, R = mesh.shape["blk"], mesh.shape["rep"]
    XN = R // 2

    def per_device(tokens, gate_weight, up_weight, down_weight):
        T, F = tokens.shape
        HW = F // 2
        PX = math.gcd(XN, HW // 128)
        PW = HW // PX
        loss_scale = float(T * B * R) ** -0.5
        dma = pltpu.SemaphoreType.DMA
        vmem = pl.BlockSpec(memory_space=pltpu.VMEM)
        row = jax.ShapeDtypeStruct((1, F), F32)
        return pl.pallas_call(
            functools.partial(kernel, B, R, PX, loss_scale),
            out_shape=(row, row, row),
            in_specs=[pl.BlockSpec(memory_space=pl.ANY), vmem, vmem, vmem],
            out_specs=(vmem, vmem, vmem),
            scratch_shapes=[
                pltpu.VMEM((T, F), BF16),
                pltpu.VMEM((2, B, 1, F), BF16),
                pltpu.VMEM((B, 1, PW), BF16),
                pltpu.VMEM((2 * B, F), F32),
                pltpu.VMEM((B, PW), F32),
                pltpu.VMEM((R, B, 128), F32),
                pltpu.VMEM((2 * B, T), F32),
                pltpu.VMEM((2 * B, HW + 128), F32),
                pltpu.VMEM((2 * B, HW + 128), F32),
                pltpu.VMEM((2 * B, HW), F32),
                pltpu.VMEM((B, PX, 2, PW + 128), BF16),
                pltpu.VMEM((B * XN, 2, PW + 128), BF16),
                pltpu.VMEM((R, 3, PW), F32),
                dma, dma((2, B)), dma((2, B)), dma((B,)), dma((B,)), dma((R,)), dma((R,)),
                dma, dma, dma((B * XN,)), dma((B * XN,)), dma((R,)), dma((R,)),
            ],
            compiler_params=pltpu.CompilerParams(collective_id=0, has_side_effects=True),
        )(tokens, gate_weight, up_weight, down_weight)

    in_specs = (P(("blk", "rep"), None), P("blk", None), P("blk", None), P("blk", None))
    out_specs = (P("blk", None), P("blk", None), P("blk", None))
    return jax.shard_map(
        per_device, mesh=mesh, in_specs=in_specs, out_specs=out_specs, check_vma=False
    )
```

```python
import functools
import math

import jax
import jax.numpy as jnp
from jax import lax
from jax.experimental import pallas as pl
from jax.experimental.pallas import tpu as pltpu
from jax.sharding import PartitionSpec as P

F32, BF16 = jnp.float32, jnp.bfloat16
NT = (((1,), (1,)), ((), ()))
EXACT = lax.Precision.HIGHEST


def each(count, body):
    if count <= 32:
        for i in range(count):
            body(i)
    else:
        lax.fori_loop(0, count, lambda i, c: (body(i), c)[1], 0)


def kernel(
    B, R, PX, loss_scale,
    tok_hbm, gate_ref, up_ref, down_ref,
    out_gate, out_up, out_down,
    tok, two, rows_in, down_in, w_all, wd_all, gram, pair, partner_in, part, send, recv, share,
    tok_sem, w_send, w_recv, f_send, f_recv, d_send, d_recv, g_send, g_recv, p_send, p_recv,
    r_send, r_recv, o_send, o_recv,
):
    T, F = tok.shape
    XN = R // 2
    HW = F // 2
    PW = HW // PX
    me_b, me_r = lax.axis_index("blk"), lax.axis_index("rep")
    core, xi = lax.rem(me_r, 2), lax.div(me_r, 2)
    everyone = PX == XN

    def if_owner(body):
        if everyone:
            body()
        else:
            pl.when(xi < PX)(body)

    def remote(src, dst, ss, rs, b, r):
        return pltpu.make_async_remote_copy(
            src_ref=src, dst_ref=dst, send_sem=ss, recv_sem=rs,
            device_id={"blk": b, "rep": r}, device_id_type=pl.DeviceIdType.MESH,
        )

    load = pltpu.make_async_copy(tok_hbm, tok, tok_sem)
    load.start()

    barrier = pltpu.get_barrier_semaphore()

    def greet(b, r):
        pl.semaphore_signal(
            barrier, inc=1, device_id={"blk": b, "rep": r}, device_id_type=pl.DeviceIdType.MESH
        )

    def same_core(i):
        k = i + 1
        return lax.rem(me_b + k // XN, B), 2 * lax.rem(xi + k % XN, XN) + core

    each(B * XN - 1, lambda i: greet(*same_core(i)))
    each(XN, lambda i: greet(me_b, 2 * i + 1 - core))

    my_col = pl.multiple_of(core * HW + lax.rem(xi, PX) * PW, 128)
    other_core = 2 * xi + 1 - core
    DW = PW // 2
    two[0:1, :] = gate_ref[...].astype(F32)
    two[1:2, :] = up_ref[...].astype(F32)
    for h in range(2):
        rows = two[:, h * HW : (h + 1) * HW]
        rows_in[me_b, h] = rows.astype(BF16)
        w_all[h, 0:2, :] = rows
    for h in range(2):
        cols = pl.ds(pl.multiple_of(my_col + h * DW, 128), DW)
        two[h : h + 1, 0:DW] = down_ref[:, cols].astype(F32)
    down_in[me_b] = two[:, 0:DW].astype(BF16)

    pl.semaphore_wait(barrier, B * XN - 1 + XN)

    def d_copy(i):
        b = lax.rem(me_b + i + 1, B)
        return remote(down_in.at[me_b], down_in.at[me_b], d_send.at[b], d_recv.at[me_b], b, me_r)

    def w_copy(i):
        b = lax.rem(me_b + i + 1, B)
        slot = rows_in.at[me_b, core]
        return remote(slot, slot, w_send.at[b], w_recv.at[me_b], b, me_r)

    def f_copy(i):
        b = lax.rem(me_b + i + 1, B)
        slot = rows_in.at[b, core]
        return remote(slot, slot, f_send.at[b], f_recv.at[b], me_b, other_core)

    each(B - 1, lambda i: d_copy(i).start())
    each(B - 1, lambda i: w_copy(i).start())

    def d_arrived(i):
        b = lax.rem(me_b + i + 1, B)
        remote(down_in.at[b], down_in.at[b], d_send.at[b], d_recv.at[b], b, me_r).wait_recv()

    each(B - 1, d_arrived)
    for k in range(B):
        for h in range(2):
            rows = down_in[lax.rem(me_b + k, B)].astype(F32)
            wd_all[k : k + 1, h * DW : (h + 1) * DW] = rows[h : h + 1]

    def g_copy(i):
        r = lax.rem(me_r + i + 1, R)
        return remote(gram.at[me_r], gram.at[me_r], g_send.at[r], g_recv.at[me_r], me_b, r)

    def make_gram():
        wd = wd_all[...].astype(BF16)
        gram[me_r, :, :] = jnp.zeros(gram.shape[1:], F32)
        gram[me_r, :, 0:B] = lax.dot_general(wd, wd, NT, preferred_element_type=F32)
        each(R - 1, lambda i: g_copy(i).start())

    if_owner(make_gram)

    def w_arrived(i):
        b = lax.rem(me_b + i + 1, B)
        slot = rows_in.at[b, core]
        remote(slot, slot, w_send.at[b], w_recv.at[b], b, me_r).wait_recv()
        f_copy(i).start()
        w_all[core, 2 * i + 2 : 2 * i + 4, :] = rows_in[b, core].astype(F32)

    def f_arrived(i):
        b = lax.rem(me_b + i + 1, B)
        slot = rows_in.at[b, 1 - core]
        remote(slot, slot, f_send.at[b], f_recv.at[b], me_b, other_core).wait_recv()
        w_all[1 - core, 2 * i + 2 : 2 * i + 4, :] = rows_in[b, 1 - core].astype(F32)

    def product(h):
        cols = pl.ds(pl.multiple_of(h * HW, 128), HW)
        return lax.dot_general(w_all[h].astype(BF16), tok[:, cols], NT, preferred_element_type=F32)

    each(B - 1, w_arrived)
    load.wait()
    first = product(core)
    each(B - 1, f_arrived)
    pair[...] = first + product(1 - core)
    gate_pre, up_pre = pair[pl.ds(0, B, stride=2), :], pair[pl.ds(1, B, stride=2), :]
    s = jax.nn.sigmoid(gate_pre)
    active = gate_pre * s
    hidden = (active * up_pre).astype(BF16)

    def g_arrived(i):
        r = lax.rem(me_r + i + 1, R)

        def wait():
            remote(gram.at[r], gram.at[r], g_send.at[r], g_recv.at[r], me_b, r).wait_recv()

        if everyone:
            wait()
        else:
            pl.when(r < 2 * PX)(wait)

    each(R - 1, g_arrived)
    gd = gram[0]
    for r in range(1, 2 * PX):
        gd = gd + gram[r]
    hidden_grad = loss_scale * jnp.dot(
        gd[:, :B], hidden.astype(F32), precision=EXACT, preferred_element_type=F32
    )
    pair[pl.ds(0, B, stride=2), :] = hidden_grad * up_pre * (s * (1.0 + gate_pre * (1.0 - s)))
    pair[pl.ds(1, B, stride=2), :] = hidden_grad * active
    lhs = pair[...].astype(BF16)

    chunk = math.gcd(512, PW)

    def terms(which, q, ref):
        for c in range(0, PW, chunk):
            col = pl.multiple_of(which * HW + q * PW + c, 128)
            ref[:, c : c + chunk] = jnp.dot(lhs, tok[:, pl.ds(col, chunk)], preferred_element_type=F32)

    def p_copy(q):
        return remote(part.at[q], partner_in.at[q], p_send.at[q], p_recv.at[q], me_b, other_core)

    for q in range(PX):
        terms(1 - core, q, part.at[q])
        part[q, :, PW:] = jnp.zeros((2 * B, 128), F32)
        if q == 0:
            turn = lax.rem(lax.broadcasted_iota(jnp.int32, (B, B), 1) + me_b, B)
            turn = turn == lax.broadcasted_iota(jnp.int32, (B, B), 0)
            named = jnp.dot(turn.astype(F32).astype(BF16), hidden, preferred_element_type=F32).astype(BF16)
            part[0, 0:B, PW : PW + B] = lax.dot_general(hidden, named, NT, preferred_element_type=F32)
            own_g = part[0, 0:B, PW:]
        p_copy(q).start()

    def r_copy(i):
        b, r = same_core(i)
        q = lax.div(r, 2)
        at = me_b * XN + xi
        qq = q if everyone else lax.rem(q, PX)
        return q, remote(send.at[lax.div(i + 1, XN), qq], recv.at[at], r_send.at[b * XN + q], r_recv.at[at], b, r)

    def for_r(act, q_now):
        def body(i):
            q, copy = r_copy(i)
            pl.when(q == q_now)(lambda: act(copy))

        each(B * XN - 1, body)

    own = part.at[PX]
    for q in range(PX):
        terms(core, q, own)
        p_copy(q).wait_recv()
        if q == 0:
            ghat = own_g + partner_in[0, 0:B, PW:]
            ghi = ghat.astype(BF16).astype(F32)
            glo = ghat - ghi
        for b in range(B):
            gpair = jnp.concatenate([ghi[b : b + 1], glo[b : b + 1]], axis=0).astype(BF16)
            term = own[2 * b : 2 * b + 2, 0:PW] + partner_in[q, 2 * b : 2 * b + 2, 0:PW]
            send[b, q, :, 0:PW] = term.astype(BF16)
            send[b, q, :, PW:] = gpair
        for_r(lambda copy: copy.start(), q)

    def o_copy(i):
        r = lax.rem(me_r + i + 1, R)
        return remote(share.at[me_r], share.at[me_r], o_send.at[r], o_recv.at[me_r], me_b, r)

    def r_arrived(i):
        b, r = same_core(i)
        at = b * XN + lax.div(r, 2)
        remote(recv.at[at], recv.at[at], r_send.at[at], r_recv.at[at], b, r).wait_recv()

    def finish():
        recv[me_b * XN + xi] = send[0, xi if everyone else lax.rem(xi, PX)]
        each(B * XN - 1, r_arrived)
        n = B * XN
        if n <= 32:
            total = recv[0].astype(F32)
            for i in range(1, n):
                total = total + recv[i].astype(F32)
        else:
            total = lax.fori_loop(
                1, n, lambda i, c: c + recv[i].astype(F32), recv[0].astype(F32)
            )
        share[me_r, 0:2, :] = total[:, 0:PW]
        grow = total[0:1, PW:] + total[1:2, PW:]
        eye = lax.rem(lax.broadcasted_iota(jnp.int32, (B, 128), 0) + me_b, B) == lax.broadcasted_iota(
            jnp.int32, (B, 128), 1
        )
        gcol = jnp.sum(jnp.where(eye, jnp.broadcast_to(grow, (B, 128)), 0.0), axis=1, keepdims=True)
        share[me_r, 2:3, :] = loss_scale * jnp.sum(gcol * wd_all[...], axis=0, keepdims=True)
        each(R - 1, lambda i: o_copy(i).start())

    if_owner(finish)

    def o_arrived(i):
        r = lax.rem(me_r + i + 1, R)

        def wait():
            remote(share.at[r], share.at[r], o_send.at[r], o_recv.at[r], me_b, r).wait_recv()

        if everyone:
            wait()
        else:
            pl.when(r < 2 * PX)(wait)

    each(R - 1, o_arrived)
    for r in range(2 * PX):
        col = (r % 2) * HW + (r // 2) * PW
        out_gate[:, col : col + PW] = share[r, 0:1, :]
        out_up[:, col : col + PW] = share[r, 1:2, :]
        out_down[:, col : col + PW] = share[r, 2:3, :]

    each(B - 1, lambda i: d_copy(i).wait_send())
    each(B - 1, lambda i: (w_copy(i).wait_send(), f_copy(i).wait_send()))
    if_owner(lambda: each(R - 1, lambda i: g_copy(i).wait_send()))
    for q in range(PX):
        p_copy(q).wait_send()
        for_r(lambda copy: copy.wait_send(), q)
    if_owner(lambda: each(R - 1, lambda i: o_copy(i).wait_send()))


def solution(mesh):
    B, R = mesh.shape["blk"], mesh.shape["rep"]
    XN = R // 2

    def per_device(tokens, gate_weight, up_weight, down_weight):
        T, F = tokens.shape
        HW = F // 2
        PX = math.gcd(XN, HW // 128)
        PW = HW // PX
        loss_scale = float(T * B * R) ** -0.5
        dma = pltpu.SemaphoreType.DMA
        vmem = pl.BlockSpec(memory_space=pltpu.VMEM)
        row = jax.ShapeDtypeStruct((1, F), F32)
        return pl.pallas_call(
            functools.partial(kernel, B, R, PX, loss_scale),
            out_shape=(row, row, row),
            in_specs=[pl.BlockSpec(memory_space=pl.ANY), vmem, vmem, vmem],
            out_specs=(vmem, vmem, vmem),
            scratch_shapes=[
                pltpu.VMEM((T, F), BF16),
                pltpu.VMEM((2, F), F32),
                pltpu.VMEM((B, 2, 2, HW), BF16),
                pltpu.VMEM((B, 2, PW // 2), BF16),
                pltpu.VMEM((2, 2 * B, HW), F32),
                pltpu.VMEM((B, PW), F32),
                pltpu.VMEM((R, B, 128), F32),
                pltpu.VMEM((2 * B, T), F32),
                pltpu.VMEM((PX, 2 * B, PW + 128), F32),
                pltpu.VMEM((PX + 1, 2 * B, PW + 128), F32),
                pltpu.VMEM((B, PX, 2, PW + 128), BF16),
                pltpu.VMEM((B * XN, 2, PW + 128), BF16),
                pltpu.VMEM((R, 3, PW), F32),
                dma, dma((B,)), dma((B,)), dma((B,)), dma((B,)), dma((B,)), dma((B,)), dma((R,)), dma((R,)),
                dma((PX,)), dma((PX,)), dma((B * XN,)), dma((B * XN,)), dma((R,)), dma((R,)),
            ],
            compiler_params=pltpu.CompilerParams(collective_id=0, has_side_effects=True),
        )(tokens, gate_weight, up_weight, down_weight)

    in_specs = (P(("blk", "rep"), None), P("blk", None), P("blk", None), P("blk", None))
    out_specs = (P("blk", None), P("blk", None), P("blk", None))
    return jax.shard_map(
        per_device, mesh=mesh, in_specs=in_specs, out_specs=out_specs, check_vma=False
    )
```

```python
import functools
import math

import jax
import jax.numpy as jnp
from jax import lax
from jax.experimental import pallas as pl
from jax.experimental.pallas import tpu as pltpu
from jax.sharding import PartitionSpec as P

F32, BF16 = jnp.float32, jnp.bfloat16
NT = (((1,), (1,)), ((), ()))
EXACT = lax.Precision.HIGHEST


def each(count, body):
    if count <= 32:
        for i in range(count):
            body(i)
    else:
        lax.fori_loop(0, count, lambda i, c: (body(i), c)[1], 0)


def kernel(
    B, R, PX, loss_scale,
    tok_hbm, gate_hbm, up_hbm, down_hbm,
    out,
    tok, gate_ref, up_ref, down_ref, two, rows_in, down_in, w_all, wd_all, gram, pair, partner_in, part, send, recv, share,
    tok_sem, in_sem, w_send, w_recv, f_send, f_recv, d_send, d_recv, g_send, g_recv, p_send, p_recv,
    r_send, r_recv, o_send, o_recv,
):
    T, F = tok.shape
    XN = R // 2
    HW = F // 2
    PW = HW // PX
    me_b, me_r = lax.axis_index("blk"), lax.axis_index("rep")
    core, xi = lax.rem(me_r, 2), lax.div(me_r, 2)
    everyone = PX == XN

    def if_owner(body):
        if everyone:
            body()
        else:
            pl.when(xi < PX)(body)

    def remote(src, dst, ss, rs, b, r):
        return pltpu.make_async_remote_copy(
            src_ref=src, dst_ref=dst, send_sem=ss, recv_sem=rs,
            device_id={"blk": b, "rep": r}, device_id_type=pl.DeviceIdType.MESH,
        )

    barrier = pltpu.get_barrier_semaphore()

    def greet(b, r):
        pl.semaphore_signal(
            barrier, inc=1, device_id={"blk": b, "rep": r}, device_id_type=pl.DeviceIdType.MESH
        )

    def far(i):
        upper = lax.div(me_b, (B + 1) // 2)
        k = 1 + lax.rem(B - 2 - me_b + upper + (2 * upper - 1) * i + B - 1, B - 1)
        return k, lax.rem(me_b + k, B)

    def same_core(i):
        k = i + 1
        return lax.rem(me_b + k // XN, B), 2 * lax.rem(xi + k % XN, XN) + core

    each(B - 1, lambda i: greet(far(i)[1], me_r))
    each(R - 1, lambda i: greet(me_b, lax.rem(me_r + i + 1, R)))
    own_rows = [
        pltpu.make_async_copy(src, dst, in_sem.at[j])
        for j, (src, dst) in enumerate(((gate_hbm, gate_ref), (up_hbm, up_ref), (down_hbm, down_ref)))
    ]
    for copy in own_rows:
        copy.start()
    load = pltpu.make_async_copy(tok_hbm, tok, tok_sem)
    load.start()

    my_col = pl.multiple_of(core * HW + lax.rem(xi, PX) * PW, 128)
    other_core = 2 * xi + 1 - core
    DW = PW // 2
    for copy in own_rows:
        copy.wait()
    two[0:1, :] = gate_ref[...].astype(F32)
    two[1:2, :] = up_ref[...].astype(F32)
    for h in range(2):
        rows = two[:, h * HW : (h + 1) * HW]
        rows_in[me_b, h] = rows.astype(BF16)
        w_all[h, 0:2, :] = rows
    for h in range(2):
        cols = pl.ds(pl.multiple_of(my_col + h * DW, 128), DW)
        two[h : h + 1, 0:DW] = down_ref[:, cols].astype(F32)
    down_in[me_b] = two[:, 0:DW].astype(BF16)

    pl.semaphore_wait(barrier, B - 1 + R - 1)

    def d_copy(i):
        b = far(i)[1]
        return remote(down_in.at[me_b], down_in.at[me_b], d_send.at[b], d_recv.at[me_b], b, me_r)

    def w_copy(i):
        b = far(i)[1]
        slot = rows_in.at[me_b, core]
        return remote(slot, slot, w_send.at[b], w_recv.at[me_b], b, me_r)

    def f_copy(i):
        b = lax.rem(me_b + i + 1, B)
        slot = rows_in.at[b, core]
        return remote(slot, slot, f_send.at[b], f_recv.at[b], me_b, other_core)

    each(B - 1, lambda i: d_copy(i).start())
    each(B - 1, lambda i: w_copy(i).start())

    def d_arrived(i):
        b = lax.rem(me_b + i + 1, B)
        remote(down_in.at[b], down_in.at[b], d_send.at[b], d_recv.at[b], b, me_r).wait_recv()

    each(B - 1, d_arrived)
    for k in range(B):
        for h in range(2):
            rows = down_in[lax.rem(me_b + k, B)].astype(F32)
            wd_all[k : k + 1, h * DW : (h + 1) * DW] = rows[h : h + 1]

    def g_copy(i):
        r = lax.rem(me_r + i + 1, R)
        return remote(gram.at[me_r], gram.at[me_r], g_send.at[r], g_recv.at[me_r], me_b, r)

    def make_gram():
        wd = wd_all[...].astype(BF16)
        gram[me_r, :, :] = jnp.zeros(gram.shape[1:], F32)
        gram[me_r, :, 0:B] = lax.dot_general(wd, wd, NT, preferred_element_type=F32)
        each(R - 1, lambda i: g_copy(i).start())

    if_owner(make_gram)

    def w_arrived(i):
        b = lax.rem(me_b + i + 1, B)
        slot = rows_in.at[b, core]
        remote(slot, slot, w_send.at[b], w_recv.at[b], b, me_r).wait_recv()
        f_copy(i).start()
        w_all[core, 2 * i + 2 : 2 * i + 4, :] = rows_in[b, core].astype(F32)

    def f_arrived(i):
        b = lax.rem(me_b + i + 1, B)
        slot = rows_in.at[b, 1 - core]
        remote(slot, slot, f_send.at[b], f_recv.at[b], me_b, other_core).wait_recv()
        w_all[1 - core, 2 * i + 2 : 2 * i + 4, :] = rows_in[b, 1 - core].astype(F32)

    def product(h):
        cols = pl.ds(pl.multiple_of(h * HW, 128), HW)
        return lax.dot_general(w_all[h].astype(BF16), tok[:, cols], NT, preferred_element_type=F32)

    each(B - 1, w_arrived)
    load.wait()
    first = product(core)
    each(B - 1, f_arrived)
    pair[...] = first + product(1 - core)
    gate_pre, up_pre = pair[pl.ds(0, B, stride=2), :], pair[pl.ds(1, B, stride=2), :]
    s = jax.nn.sigmoid(gate_pre)
    active = gate_pre * s
    hidden = (active * up_pre).astype(BF16)

    def g_arrived(i):
        r = lax.rem(me_r + i + 1, R)

        def wait():
            remote(gram.at[r], gram.at[r], g_send.at[r], g_recv.at[r], me_b, r).wait_recv()

        if everyone:
            wait()
        else:
            pl.when(r < 2 * PX)(wait)

    each(R - 1, g_arrived)
    gd = gram[0]
    for r in range(1, 2 * PX):
        gd = gd + gram[r]
    hidden_grad = loss_scale * jnp.dot(
        gd[:, :B], hidden.astype(F32), precision=EXACT, preferred_element_type=F32
    )
    pair[pl.ds(0, B, stride=2), :] = hidden_grad * up_pre * (s * (1.0 + gate_pre * (1.0 - s)))
    pair[pl.ds(1, B, stride=2), :] = hidden_grad * active
    lhs = pair[...].astype(BF16)

    chunk = math.gcd(512, PW)

    def terms(which, q, ref):
        for c in range(0, PW, chunk):
            col = pl.multiple_of(which * HW + q * PW + c, 128)
            ref[:, c : c + chunk] = jnp.dot(lhs, tok[:, pl.ds(col, chunk)], preferred_element_type=F32)

    def p_copy(q):
        return remote(part.at[q], partner_in.at[q], p_send.at[q], p_recv.at[q], me_b, other_core)

    turns = [lax.rem(xi + 1 + j, PX) for j in range(PX)]
    for j, q in enumerate(turns):
        terms(1 - core, q, part.at[j])
        part[j, :, PW:] = jnp.zeros((2 * B, 128), F32)
        if j == 0:
            turn = lax.rem(lax.broadcasted_iota(jnp.int32, (B, B), 1) + me_b, B)
            turn = turn == lax.broadcasted_iota(jnp.int32, (B, B), 0)
            named = jnp.dot(turn.astype(F32).astype(BF16), hidden, preferred_element_type=F32).astype(BF16)
            part[0, 0:B, PW : PW + B] = lax.dot_general(hidden, named, NT, preferred_element_type=F32)
            own_g = part[0, 0:B, PW:]
        p_copy(j).start()

    at = me_b * XN + xi

    def for_r(act, j):
        q = turns[j]

        def to(k, b):
            act(
                remote(
                    send.at[j, k], recv.at[at], r_send.at[j, k], r_recv.at[at], b, 2 * q + core
                )
            )

        each(B - 1, lambda i: to(*far(i)))
        if not everyone:
            pl.when(q != xi)(lambda: to(0, me_b))
        elif j < PX - 1:
            to(0, me_b)

    own = part.at[PX]
    for j, q in enumerate(turns):
        terms(core, q, own)
        p_copy(j).wait_recv()
        if j == 0:
            ghat = own_g + partner_in[0, 0:B, PW:]
            ghi = ghat.astype(BF16).astype(F32)
            glo = ghat - ghi
        for b in range(B):
            gpair = jnp.concatenate([ghi[b : b + 1], glo[b : b + 1]], axis=0).astype(BF16)
            term = own[2 * b : 2 * b + 2, 0:PW] + partner_in[j, 2 * b : 2 * b + 2, 0:PW]
            send[j, b, :, 0:PW] = term.astype(BF16)
            send[j, b, :, PW:] = gpair
        for_r(lambda copy: copy.start(), j)

    def columns(r):
        return out.at[:, :, pl.ds(pl.multiple_of(lax.rem(r, 2) * HW + lax.div(r, 2) * PW, 128), PW)]

    def o_copy(i):
        r = lax.rem(me_r + 1 + lax.rem(i + 1, R - 1), R)
        return remote(share, columns(me_r), o_send.at[r], o_recv.at[me_r], me_b, r)

    def r_arrived(i):
        b, r = same_core(i)
        n = b * XN + lax.div(r, 2)
        remote(recv.at[n], recv.at[n], r_send.at[0, 0], r_recv.at[n], b, r).wait_recv()

    def finish():
        recv[at] = send[PX - 1, 0]
        each(B * XN - 1, r_arrived)
        n = B * XN
        if n <= 32:
            total = recv[0].astype(F32)
            for i in range(1, n):
                total = total + recv[i].astype(F32)
        else:
            total = lax.fori_loop(
                1, n, lambda i, c: c + recv[i].astype(F32), recv[0].astype(F32)
            )
        share[0] = total[0:1, 0:PW]
        share[1] = total[1:2, 0:PW]
        grow = total[0:1, PW:] + total[1:2, PW:]
        eye = lax.rem(lax.broadcasted_iota(jnp.int32, (B, 128), 0) + me_b, B) == lax.broadcasted_iota(
            jnp.int32, (B, 128), 1
        )
        gcol = jnp.sum(jnp.where(eye, jnp.broadcast_to(grow, (B, 128)), 0.0), axis=1, keepdims=True)
        share[2] = loss_scale * jnp.sum(gcol * wd_all[...], axis=0, keepdims=True)
        each(R - 1, lambda i: o_copy(i).start())
        pltpu.make_async_copy(share, columns(me_r), in_sem.at[0]).start()

    if_owner(finish)

    def o_arrived(i):
        r = lax.rem(me_r + i + 1, R)

        def wait():
            remote(columns(r), columns(r), o_send.at[r], o_recv.at[r], me_b, r).wait_recv()

        if everyone:
            wait()
        else:
            pl.when(r < 2 * PX)(wait)

    each(R - 1, o_arrived)
    each(B - 1, lambda i: d_copy(i).wait_send())
    each(B - 1, lambda i: (w_copy(i).wait_send(), f_copy(i).wait_send()))
    if_owner(lambda: each(R - 1, lambda i: g_copy(i).wait_send()))
    for j in range(PX):
        p_copy(j).wait_send()
        for_r(lambda copy: copy.wait_send(), j)

    def left():
        each(R - 1, lambda i: o_copy(i).wait_send())
        pltpu.make_async_copy(share, columns(me_r), in_sem.at[0]).wait()

    if_owner(left)


def solution(mesh):
    B, R = mesh.shape["blk"], mesh.shape["rep"]
    XN = R // 2

    def per_device(tokens, gate_weight, up_weight, down_weight):
        T, F = tokens.shape
        HW = F // 2
        PX = math.gcd(XN, HW // 128)
        PW = HW // PX
        loss_scale = float(T * B * R) ** -0.5
        dma = pltpu.SemaphoreType.DMA
        hbm = pl.BlockSpec(memory_space=pl.ANY)

        out = pl.pallas_call(
            functools.partial(kernel, B, R, PX, loss_scale),
            out_shape=jax.ShapeDtypeStruct((3, 1, F), F32),
            in_specs=[hbm] * 4,
            out_specs=hbm,
            scratch_shapes=[
                pltpu.VMEM((T, F), BF16),
                pltpu.VMEM((1, F), BF16),
                pltpu.VMEM((1, F), BF16),
                pltpu.VMEM((1, F), BF16),
                pltpu.VMEM((2, F), F32),
                pltpu.VMEM((B, 2, 2, HW), BF16),
                pltpu.VMEM((B, 2, PW // 2), BF16),
                pltpu.VMEM((2, 2 * B, HW), F32),
                pltpu.VMEM((B, PW), F32),
                pltpu.VMEM((R, B, 128), F32),
                pltpu.VMEM((2 * B, T), F32),
                pltpu.VMEM((PX, 2 * B, PW + 128), F32),
                pltpu.VMEM((PX + 1, 2 * B, PW + 128), F32),
                pltpu.VMEM((PX, B, 2, PW + 128), BF16),
                pltpu.VMEM((B * XN, 2, PW + 128), BF16),
                pltpu.VMEM((3, 1, PW), F32),
                dma, dma((3,)), dma((B,)), dma((B,)), dma((B,)), dma((B,)), dma((B,)), dma((B,)), dma((R,)), dma((R,)),
                dma((PX,)), dma((PX,)), dma((PX, B)), dma((B * XN,)), dma((R,)), dma((R,)),
            ],
            compiler_params=pltpu.CompilerParams(collective_id=0, has_side_effects=True),
        )(tokens, gate_weight, up_weight, down_weight)
        return out[0], out[1], out[2]

    in_specs = (P(("blk", "rep"), None), P("blk", None), P("blk", None), P("blk", None))
    out_specs = (P("blk", None), P("blk", None), P("blk", None))
    return jax.shard_map(
        per_device, mesh=mesh, in_specs=in_specs, out_specs=out_specs, check_vma=False
    )
```

```python
import functools
import math

import jax
import jax.numpy as jnp
from jax import lax
from jax.experimental import pallas as pl
from jax.experimental.pallas import tpu as pltpu
from jax.sharding import PartitionSpec as P

F32, BF16 = jnp.float32, jnp.bfloat16
NT = (((1,), (1,)), ((), ()))
EXACT = lax.Precision.HIGHEST


def each(count, body):
    if count <= 32:
        for i in range(count):
            body(i)
    else:
        lax.fori_loop(0, count, lambda i, c: (body(i), c)[1], 0)


def kernel(
    B, R, PX, loss_scale,
    tok_hbm, gate_hbm, up_hbm, down_hbm,
    out,
    tok, gate_ref, up_ref, down_ref, two, rows_in, down_in, w_all, wd_all, gram, pair, partner_in, part, send, recv, share,
    tok_sem, in_sem, w_send, w_recv, f_send, f_recv, d_send, d_recv, g_send, g_recv, p_send, p_recv,
    r_send, r_recv, o_send, o_recv,
):
    T, F = tok.shape
    XN = R // 2
    HW = F // 2
    PW = HW // PX
    me_b, me_r = lax.axis_index("blk"), lax.axis_index("rep")
    core, xi = lax.rem(me_r, 2), lax.div(me_r, 2)
    everyone = PX == XN

    def if_owner(body):
        if everyone:
            body()
        else:
            pl.when(xi < PX)(body)

    def remote(src, dst, ss, rs, b, r):
        return pltpu.make_async_remote_copy(
            src_ref=src, dst_ref=dst, send_sem=ss, recv_sem=rs,
            device_id={"blk": b, "rep": r}, device_id_type=pl.DeviceIdType.MESH,
        )

    barrier = pltpu.get_barrier_semaphore()

    def greet(b, r):
        pl.semaphore_signal(
            barrier, inc=1, device_id={"blk": b, "rep": r}, device_id_type=pl.DeviceIdType.MESH
        )

    def far(i):
        upper = lax.div(me_b, (B + 1) // 2)
        k = 1 + lax.rem(B - 2 - me_b + upper + (2 * upper - 1) * i + B - 1, B - 1)
        return k, lax.rem(me_b + k, B)

    def same_core(i):
        k = i + 1
        return lax.rem(me_b + k // XN, B), 2 * lax.rem(xi + k % XN, XN) + core

    each(B - 1, lambda i: greet(far(i)[1], me_r))
    each(R - 1, lambda i: greet(me_b, lax.rem(me_r + i + 1, R)))
    own_rows = [
        pltpu.make_async_copy(src, dst, in_sem.at[j])
        for j, (src, dst) in enumerate(((gate_hbm, gate_ref), (up_hbm, up_ref), (down_hbm, down_ref)))
    ]
    for copy in own_rows:
        copy.start()
    load = pltpu.make_async_copy(tok_hbm, tok, tok_sem)
    load.start()

    my_col = pl.multiple_of(core * HW + lax.rem(xi, PX) * PW, 128)
    other_core = 2 * xi + 1 - core
    DW = PW // 2
    for copy in own_rows:
        copy.wait()
    two[0:1, :] = gate_ref[...].astype(F32)
    two[1:2, :] = up_ref[...].astype(F32)
    for h in range(2):
        rows = two[:, h * HW : (h + 1) * HW]
        rows_in[me_b, h] = rows.astype(BF16)
        w_all[h, 0:2, :] = rows
    for h in range(2):
        cols = pl.ds(pl.multiple_of(my_col + h * DW, 128), DW)
        two[h : h + 1, 0:DW] = down_ref[:, cols].astype(F32)
    down_in[me_b] = two[:, 0:DW].astype(BF16)

    pl.semaphore_wait(barrier, B - 1 + R - 1)

    def d_copy(i):
        b = far(i)[1]
        return remote(down_in.at[me_b], down_in.at[me_b], d_send.at[b], d_recv.at[me_b], b, me_r)

    def w_copy(i):
        b = far(i)[1]
        slot = rows_in.at[me_b, core]
        return remote(slot, slot, w_send.at[b], w_recv.at[me_b], b, me_r)

    def f_copy(i):
        b = lax.rem(me_b + i + 1, B)
        slot = rows_in.at[b, core]
        return remote(slot, slot, f_send.at[b], f_recv.at[b], me_b, other_core)

    each(B - 1, lambda i: d_copy(i).start())
    each(B - 1, lambda i: w_copy(i).start())

    def d_arrived(i):
        b = lax.rem(me_b + i + 1, B)
        remote(down_in.at[b], down_in.at[b], d_send.at[b], d_recv.at[b], b, me_r).wait_recv()

    each(B - 1, d_arrived)
    for k in range(B):
        for h in range(2):
            rows = down_in[lax.rem(me_b + k, B)].astype(F32)
            wd_all[k : k + 1, h * DW : (h + 1) * DW] = rows[h : h + 1]

    def g_copy(i):
        r = lax.rem(me_r + i + 1, R)
        return remote(gram.at[me_r], gram.at[me_r], g_send.at[r], g_recv.at[me_r], me_b, r)

    def make_gram():
        wd = wd_all[...].astype(BF16)
        gram[me_r, :, :] = jnp.zeros(gram.shape[1:], F32)
        gram[me_r, :, 0:B] = lax.dot_general(wd, wd, NT, preferred_element_type=F32)
        each(R - 1, lambda i: g_copy(i).start())

    if_owner(make_gram)

    def w_arrived(i):
        b = lax.rem(me_b + i + 1, B)
        slot = rows_in.at[b, core]
        remote(slot, slot, w_send.at[b], w_recv.at[b], b, me_r).wait_recv()
        f_copy(i).start()
        w_all[core, 2 * i + 2 : 2 * i + 4, :] = rows_in[b, core].astype(F32)

    def f_arrived(i):
        b = lax.rem(me_b + i + 1, B)
        slot = rows_in.at[b, 1 - core]
        remote(slot, slot, f_send.at[b], f_recv.at[b], me_b, other_core).wait_recv()
        w_all[1 - core, 2 * i + 2 : 2 * i + 4, :] = rows_in[b, 1 - core].astype(F32)

    def product(h):
        cols = pl.ds(pl.multiple_of(h * HW, 128), HW)
        return lax.dot_general(w_all[h].astype(BF16), tok[:, cols], NT, preferred_element_type=F32)

    each(B - 1, w_arrived)
    load.wait()
    first = product(core)
    each(B - 1, f_arrived)
    pair[...] = first + product(1 - core)
    gate_pre, up_pre = pair[pl.ds(0, B, stride=2), :], pair[pl.ds(1, B, stride=2), :]
    s = jax.nn.sigmoid(gate_pre)
    active = gate_pre * s
    hidden = (active * up_pre).astype(BF16)

    def g_arrived(i):
        r = lax.rem(me_r + i + 1, R)

        def wait():
            remote(gram.at[r], gram.at[r], g_send.at[r], g_recv.at[r], me_b, r).wait_recv()

        if everyone:
            wait()
        else:
            pl.when(r < 2 * PX)(wait)

    each(R - 1, g_arrived)
    gd = gram[0]
    for r in range(1, 2 * PX):
        gd = gd + gram[r]
    hidden_grad = loss_scale * jnp.dot(
        gd[:, :B], hidden.astype(F32), precision=EXACT, preferred_element_type=F32
    )
    pair[pl.ds(0, B, stride=2), :] = hidden_grad * up_pre * (s * (1.0 + gate_pre * (1.0 - s)))
    pair[pl.ds(1, B, stride=2), :] = hidden_grad * active
    lhs = pair[...].astype(BF16)

    chunk = math.gcd(512, PW)

    def terms(which, q, ref):
        for c in range(0, PW, chunk):
            col = pl.multiple_of(which * HW + q * PW + c, 128)
            ref[:, c : c + chunk] = jnp.dot(lhs, tok[:, pl.ds(col, chunk)], preferred_element_type=F32)

    def p_copy(q):
        return remote(part.at[q], partner_in.at[q], p_send.at[q], p_recv.at[q], me_b, other_core)

    turns = [lax.rem(xi + 1 + j, PX) for j in range(PX)]
    for j, q in enumerate(turns):
        terms(1 - core, q, part.at[j])
        part[j, :, PW:] = jnp.zeros((2 * B, 128), F32)
        if j == 0:
            turn = lax.rem(lax.broadcasted_iota(jnp.int32, (B, B), 1) + me_b, B)
            turn = turn == lax.broadcasted_iota(jnp.int32, (B, B), 0)
            named = jnp.dot(turn.astype(F32).astype(BF16), hidden, preferred_element_type=F32).astype(BF16)
            part[0, 0:B, PW : PW + B] = lax.dot_general(hidden, named, NT, preferred_element_type=F32)
            own_g = part[0, 0:B, PW:]
        p_copy(j).start()

    at = me_b * XN + xi

    def for_r(act, j):
        q = turns[j]

        def to(k, b):
            act(
                remote(
                    send.at[j, k], recv.at[at], r_send.at[j, k], r_recv.at[at], b, 2 * q + core
                )
            )

        each(B - 1, lambda i: to(*far(i)))
        if not everyone:
            pl.when(q != xi)(lambda: to(0, me_b))
        elif j < PX - 1:
            to(0, me_b)

    own = part.at[PX]
    for j, q in enumerate(turns):
        terms(core, q, own)
        p_copy(j).wait_recv()
        if j == 0:
            ghat = own_g + partner_in[0, 0:B, PW:]
            ghi = ghat.astype(BF16).astype(F32)
            glo = ghat - ghi
        for b in range(B):
            gpair = jnp.concatenate([ghi[b : b + 1], glo[b : b + 1]], axis=0).astype(BF16)
            term = own[2 * b : 2 * b + 2, 0:PW] + partner_in[j, 2 * b : 2 * b + 2, 0:PW]
            send[j, b, :, 0:PW] = term.astype(BF16)
            send[j, b, :, PW:] = gpair
        for_r(lambda copy: copy.start(), j)

    def columns(r):
        return out.at[:, :, pl.ds(pl.multiple_of(lax.rem(r, 2) * HW + lax.div(r, 2) * PW, 128), PW)]

    def o_copy(i):
        r = lax.rem(me_r + 1 + lax.rem(i + 1, R - 1), R)
        return remote(share, columns(me_r), o_send.at[r], o_recv.at[me_r], me_b, r)

    def r_arrived(i):
        b, r = same_core(i)
        n = b * XN + lax.div(r, 2)
        remote(recv.at[n], recv.at[n], r_send.at[0, 0], r_recv.at[n], b, r).wait_recv()

    def finish():
        recv[at] = send[PX - 1, 0]
        each(B * XN - 1, r_arrived)
        n = B * XN
        if n <= 32:
            total = recv[0].astype(F32)
            for i in range(1, n):
                total = total + recv[i].astype(F32)
        else:
            total = lax.fori_loop(
                1, n, lambda i, c: c + recv[i].astype(F32), recv[0].astype(F32)
            )
        share[0] = total[0:1, 0:PW]
        share[1] = total[1:2, 0:PW]
        grow = total[0:1, PW:] + total[1:2, PW:]
        eye = lax.rem(lax.broadcasted_iota(jnp.int32, (B, 128), 0) + me_b, B) == lax.broadcasted_iota(
            jnp.int32, (B, 128), 1
        )
        gcol = jnp.sum(jnp.where(eye, jnp.broadcast_to(grow, (B, 128)), 0.0), axis=1, keepdims=True)
        share[2] = loss_scale * jnp.sum(gcol * wd_all[...], axis=0, keepdims=True)
        each(R - 1, lambda i: o_copy(i).start())
        pltpu.make_async_copy(share, columns(me_r), in_sem.at[0]).start()

    if_owner(finish)

    def o_arrived(i):
        r = lax.rem(me_r + i + 1, R)

        def wait():
            remote(columns(r), columns(r), o_send.at[r], o_recv.at[r], me_b, r).wait_recv()

        if everyone:
            wait()
        else:
            pl.when(r < 2 * PX)(wait)

    each(R - 1, o_arrived)
    each(B - 1, lambda i: d_copy(i).wait_send())
    each(B - 1, lambda i: (w_copy(i).wait_send(), f_copy(i).wait_send()))
    if_owner(lambda: each(R - 1, lambda i: g_copy(i).wait_send()))
    for j in range(PX):
        p_copy(j).wait_send()
        for_r(lambda copy: copy.wait_send(), j)

    def left():
        each(R - 1, lambda i: o_copy(i).wait_send())
        pltpu.make_async_copy(share, columns(me_r), in_sem.at[0]).wait()

    if_owner(left)


def solution(mesh):
    B, R = mesh.shape["blk"], mesh.shape["rep"]
    XN = R // 2

    def per_device(tokens, gate_weight, up_weight, down_weight):
        T, F = tokens.shape
        HW = F // 2
        PX = math.gcd(XN, HW // 128)
        PW = HW // PX
        loss_scale = float(T * B * R) ** -0.5
        dma = pltpu.SemaphoreType.DMA
        hbm = pl.BlockSpec(memory_space=pl.ANY)

        out = pl.pallas_call(
            functools.partial(kernel, B, R, PX, loss_scale),
            out_shape=pltpu.VMEM((3, 1, F), F32),
            in_specs=[hbm] * 4,
            out_specs=pl.BlockSpec(memory_space=pltpu.VMEM),
            scratch_shapes=[
                pltpu.VMEM((T, F), BF16),
                pltpu.VMEM((1, F), BF16),
                pltpu.VMEM((1, F), BF16),
                pltpu.VMEM((1, F), BF16),
                pltpu.VMEM((2, F), F32),
                pltpu.VMEM((B, 2, 2, HW), BF16),
                pltpu.VMEM((B, 2, PW // 2), BF16),
                pltpu.VMEM((2, 2 * B, HW), F32),
                pltpu.VMEM((B, PW), F32),
                pltpu.VMEM((R, B, 128), F32),
                pltpu.VMEM((2 * B, T), F32),
                pltpu.VMEM((PX, 2 * B, PW + 128), F32),
                pltpu.VMEM((PX + 1, 2 * B, PW + 128), F32),
                pltpu.VMEM((PX, B, 2, PW + 128), BF16),
                pltpu.VMEM((B * XN, 2, PW + 128), BF16),
                pltpu.VMEM((3, 1, PW), F32),
                dma, dma((3,)), dma((B,)), dma((B,)), dma((B,)), dma((B,)), dma((B,)), dma((B,)), dma((R,)), dma((R,)),
                dma((PX,)), dma((PX,)), dma((PX, B)), dma((B * XN,)), dma((R,)), dma((R,)),
            ],
            compiler_params=pltpu.CompilerParams(collective_id=0, has_side_effects=True),
        )(tokens, gate_weight, up_weight, down_weight)
        return out[0], out[1], out[2]

    in_specs = (P(("blk", "rep"), None), P("blk", None), P("blk", None), P("blk", None))
    out_specs = (P("blk", None), P("blk", None), P("blk", None))
    return jax.shard_map(
        per_device, mesh=mesh, in_specs=in_specs, out_specs=out_specs, check_vma=False
    )
```
